8 devices in a mesh: depth: 2 (over z, y), col: 2 (over x), row: 2 (over core).
Axes of the slice: x: 2, y: 2, z: 1, core: 2. Of those that a mesh axis runs over, the one named last changes fastest.
Arguments:
- tokens: bfloat16 [4096, 4096], P(('depth', 'row'), 'col')
- w_up: bfloat16 [4096, 16384], P('row', 'col')
- w_down: bfloat16 [16384, 4096], P('row', 'col')
- grad_out: bfloat16 [4096, 4096], P(('depth', 'row'), 'col')
Outputs:
- output 1: bfloat16 [4096, 4096], P(('depth', 'row'), 'col')
- output 2: bfloat16 [4096, 4096], P(('depth', 'row'), 'col')
- output 3: float32 [4096, 16384], P('row', 'col')
- output 4: float32 [16384, 4096], P('row', 'col')
All inputs are finite; a program needn't handle non-finite values.
Results may differ from the reference program's by a relative error of at most 0.001.
Values are sent between devices in bfloat16 or wider.
A program may use at most 1 GiB of HBM per device.

```python
import math
import jax
import jax.numpy as jnp
from jax import lax

TOKENS_DEV = 1024
HIDDEN = 4096
FFN_WIDTH = 16384
BLOCKS = 4
TOKENS = TOKENS_DEV * BLOCKS
INV_ROOT_TWO = 1.0 / math.sqrt(2.0)
INV_ROOT_TAU = 1.0 / math.sqrt(2.0 * math.pi)


def setup_inputs(seed: int = 0) -> dict:
    base_key = jax.random.key(seed)
    key_tok, key_up, key_down, key_grad = jax.random.split(base_key, 4)
    tokens = jax.random.normal(key_tok, (TOKENS, HIDDEN), jnp.float32)
    w_up = jax.random.normal(key_up, (HIDDEN, FFN_WIDTH), jnp.float32) * (HIDDEN ** -0.5)
    w_down = jax.random.normal(key_down, (FFN_WIDTH, HIDDEN), jnp.float32) * (FFN_WIDTH ** -0.5)
    grad_out = jax.random.normal(key_grad, (TOKENS, HIDDEN), jnp.float32)
    return {"tokens": tokens.astype(jnp.bfloat16), "w_up": w_up.astype(jnp.bfloat16), "w_down": w_down.astype(jnp.bfloat16), "grad_out": grad_out.astype(jnp.bfloat16)}


def gelu_value(pre_act):
    return 0.5 * pre_act * (1.0 + lax.erf(pre_act * INV_ROOT_TWO))


def gelu_slope(pre_act):
    return 0.5 * (1.0 + lax.erf(pre_act * INV_ROOT_TWO)) + pre_act * jnp.exp(-0.5 * pre_act * pre_act) * INV_ROOT_TAU


def reference(tokens, w_up, w_down, grad_out):
    tok_blocks = tokens.reshape(BLOCKS, TOKENS_DEV, HIDDEN)
    grad_blocks = grad_out.reshape(BLOCKS, TOKENS_DEV, HIDDEN)

    def one_block(acc_pair, blk_pair):
        acc_up, acc_down = acc_pair
        tok_blk, grad_blk = blk_pair
        pre_act = jnp.dot(tok_blk, w_up, preferred_element_type=jnp.float32)
        hidden_act = gelu_value(pre_act).astype(jnp.bfloat16)
        out_blk = jnp.dot(hidden_act, w_down, preferred_element_type=jnp.float32).astype(jnp.bfloat16)
        grad_act = jnp.dot(grad_blk, w_down.T, preferred_element_type=jnp.float32)
        grad_pre = (grad_act * gelu_slope(pre_act)).astype(jnp.bfloat16)
        grad_tok = jnp.dot(grad_pre, w_up.T, preferred_element_type=jnp.float32).astype(jnp.bfloat16)
        acc_down = acc_down + jnp.dot(hidden_act.T, grad_blk, preferred_element_type=jnp.float32)
        acc_up = acc_up + jnp.dot(tok_blk.T, grad_pre, preferred_element_type=jnp.float32)
        return (acc_up, acc_down), (out_blk, grad_tok)

    start_acc = (jnp.zeros((HIDDEN, FFN_WIDTH), jnp.float32), jnp.zeros((FFN_WIDTH, HIDDEN), jnp.float32))
    (grad_w_up, grad_w_down), (out_blocks, grad_tok_blocks) = lax.scan(one_block, start_acc, (tok_blocks, grad_blocks))
    return (out_blocks.reshape(TOKENS, HIDDEN), grad_tok_blocks.reshape(TOKENS, HIDDEN), grad_w_up, grad_w_down)
```

```python
import math
import jax
import jax.numpy as jnp
from jax import lax
from jax.sharding import PartitionSpec as P

INV_ROOT_TWO = 1.0 / math.sqrt(2.0)
INV_ROOT_TAU = 1.0 / math.sqrt(2.0 * math.pi)
SWAP = [(0, 1), (1, 0)]
PIECES = 4


def gelu_value(pre_act):
    return 0.5 * pre_act * (1.0 + lax.erf(pre_act * INV_ROOT_TWO))


def gelu_slope(pre_act):
    return 0.5 * (1.0 + lax.erf(pre_act * INV_ROOT_TWO)) + pre_act * jnp.exp(-0.5 * pre_act * pre_act) * INV_ROOT_TAU


def dot(a, b, eq, add=None):
    out = jnp.einsum(eq, a, b, preferred_element_type=jnp.float32)
    return lax.optimization_barrier(out if add is None else out + add)


def forward(a, b):
    pre = jnp.einsum("th,hf->tf", a, b, preferred_element_type=jnp.float32)
    return lax.optimization_barrier((pre, gelu_value(pre).astype(jnp.bfloat16)))


def backward(a, b, add, pre):
    out = jnp.einsum("th,fh->tf", a, b, preferred_element_type=jnp.float32) + add
    return lax.optimization_barrier((out * gelu_slope(pre)).astype(jnp.bfloat16))


def swap(x, axis):
    return lax.ppermute(x, axis, SWAP)


def solution(mesh):
    act_spec = P(("depth", "row"), "col")
    wgt_spec = P("row", "col")

    def grid_block(tok, up, down, grad):
        layer, col, row = lax.axis_index("depth"), lax.axis_index("col"), lax.axis_index("row")
        half = tok.shape[1]
        wide = up.shape[1]
        diag = row == col

        def join(a, b):
            return jnp.where(col == 0, jnp.concatenate([a, b], 1), jnp.concatenate([b, a], 1))

        q = wide // 2
        sub = lax.dynamic_slice(down, (row * q, layer * (half // 2)), (q, half // 2))
        oth = swap(lax.dynamic_slice(down, ((1 - row) * q, layer * (half // 2)), (q, half // 2)), "row")
        piece = jnp.where(diag, oth, sub)

        tok_1 = swap(tok, "col")
        tok_2 = swap(tok, "depth")
        grad_1 = swap(grad, "col")
        grad_2 = swap(grad, "depth")
        up_g = lax.all_gather(up, "row", axis=0, tiled=True)
        down_g = lax.all_gather(down, "row", axis=0, tiled=True)
        e = q // 2
        p1a, p1b = swap(piece[:e], "col"), swap(piece[e:], "col")
        p2a, p2b = swap(p1a, "depth"), swap(p1b, "depth")
        p1, p2 = jnp.concatenate([p1a, p1b], 0), jnp.concatenate([p2a, p2b], 0)
        tok_3 = swap(tok_1, "depth")
        grad_3 = swap(grad_1, "depth")
        down_a = lax.all_gather(p1, "row", axis=0, tiled=True)
        down_b = lax.all_gather(p2, "row", axis=0, tiled=True)
        down_c = lax.dynamic_slice_in_dim(down_g, col * wide, wide, 0)
        down_n = lax.dynamic_slice_in_dim(down_g, (1 - col) * wide, wide, 0)
        tok_h = join(tok, tok_1)
        tok_t = join(tok_2, tok_3)

        pre_h, act_h = forward(tok_h, up_g)
        pre_t, act_t = forward(tok_t, up_g)

        w = wide // PIECES
        cut = lambda x, j: x[:, j * w:(j + 1) * w]
        imp_h = [swap(cut(act_h, j), "col") for j in range(PIECES)]
        imp_t = [swap(imp_h[j], "depth") for j in range(PIECES)]

        first = lambda g: lax.dynamic_slice_in_dim(g, layer * (half // 2), half // 2, 1)
        second = lambda g: lax.dynamic_slice_in_dim(g, (1 - layer) * (half // 2), half // 2, 1)
        dh = dot(grad, down_c, "th,fh->tf")
        dh = dot(first(grad_1), down_a, "th,fh->tf", dh)
        du_h = backward(second(grad_1), down_b, dh, pre_h)
        part = dot(du_h, up_g, "tf,hf->th")
        away = swap(lax.dynamic_slice_in_dim(part, (1 - col) * half, half, 1), "col")
        grad_tok = (lax.dynamic_slice_in_dim(part, col * half, half, 1) + away).astype(jnp.bfloat16)
        dt = dot(grad_2, down_c, "th,fh->tf")
        dt = dot(first(grad_3), down_a, "th,fh->tf", dt)
        du_t = backward(second(grad_3), down_b, dt, pre_t)

        cols = lambda x, k: lax.dynamic_slice_in_dim(x, k * half, half, 1)
        tok_sh, tok_st = swap(cols(tok_h, 1 - row), "row"), swap(cols(tok_t, 1 - row), "row")
        du_sh, du_st = swap(du_h, "row"), swap(du_t, "row")
        up_sum = dot(cols(tok_h, row), du_h, "th,tf->hf")
        up_sum = dot(tok_sh, du_sh, "th,tf->hf", up_sum)
        up_sum = dot(cols(tok_t, row), du_t, "th,tf->hf", up_sum)
        up_sum = dot(tok_st, du_st, "th,tf->hf", up_sum)

        imp_ha = jnp.concatenate(imp_h, 1)
        imp_ta = jnp.concatenate(imp_t, 1)
        out = dot(act_h, down_c, "tf,fh->th")
        out = dot(imp_ha, down_n, "tf,fh->th", out).astype(jnp.bfloat16)

        grad_sh, grad_st = swap(grad, "row"), swap(grad_2, "row")
        oth_h = swap(jnp.where(diag, imp_ha, act_h), "row")
        oth_t = swap(jnp.where(diag, imp_ta, act_t), "row")
        down_sum = dot(jnp.where(diag, act_h, imp_ha), grad, "tf,th->fh")
        down_sum = dot(oth_h, grad_sh, "tf,th->fh", down_sum)
        down_sum = dot(jnp.where(diag, act_t, imp_ta), grad_2, "tf,th->fh", down_sum)
        down_sum = dot(oth_t, grad_st, "tf,th->fh", down_sum)
        return out, grad_tok, up_sum, down_sum

    return jax.shard_map(grid_block, mesh=mesh, in_specs=(act_spec, wgt_spec, wgt_spec, act_spec), out_specs=(act_spec, act_spec, wgt_spec, wgt_spec), check_vma=False)
```

```python
import functools
import math
import jax
import jax.numpy as jnp
from jax import lax
from jax.experimental import pallas as pl
from jax.experimental.pallas import tpu as pltpu
from jax.sharding import PartitionSpec as P

INV_ROOT_TWO = 1.0 / math.sqrt(2.0)
INV_ROOT_TAU = 1.0 / math.sqrt(2.0 * math.pi)
SWAP = [(0, 1), (1, 0)]
PIECES = 4
PARTS = 2


ANY = pl.BlockSpec(memory_space=pl.ANY)
F32, BF16 = jnp.float32, jnp.bfloat16

TN = (((0,), (0,)), ((), ()))
NN = (((1,), (0,)), ((), ()))
NT = (((1,), (1,)), ((), ()))


def cost(m, n, k):
    return pl.CostEstimate(flops=2 * m * n * k, bytes_accessed=2 * (m * k + n * k) + 4 * m * n, transcendentals=0)


def up_kernel(x0, x1, x2, x3, d0, d1, d2, d3, out, lhs, sem):
    depth = x0.shape[1]
    copies = [pltpu.make_async_copy(x, lhs.at[:, pl.ds(k * depth, depth)], sem.at[k]) for k, x in enumerate((x0, x1, x2, x3))]

    @pl.when(pl.program_id(0) == 0)
    def _():
        for c in copies:
            c.start()
        for c in copies:
            c.wait()

    total = None
    for k, d in enumerate((d0, d1, d2, d3)):
        part = lax.dot_general(lhs[:, k * depth:(k + 1) * depth], d[...], NN, preferred_element_type=jnp.float32)
        total = part if total is None else total + part
    out[...] = total


def up_grad(xs, ds, bn=512):
    m, depth = xs[0].shape
    n = ds[0].shape[1]
    return pl.pallas_call(
        up_kernel,
        grid=(n // bn,),
        out_shape=jax.ShapeDtypeStruct((m, n), jnp.float32),
        in_specs=[pl.BlockSpec(memory_space=pl.ANY)] * 4 + [pl.BlockSpec((depth, bn), lambda i: (0, i))] * 4,
        out_specs=pl.BlockSpec((m, bn), lambda i: (0, i)),
        scratch_shapes=[pltpu.VMEM((m, 4 * depth), jnp.bfloat16), pltpu.SemaphoreType.DMA((4,))],
        compiler_params=params(),
        cost_estimate=cost(m, n, 4 * depth),
        name="up_grad",
    )(*xs, *ds)


def down_kernel(pieces, *refs):
    act_h, act_t, imp_h, imp_t, oth_h, oth_t = [refs[n * pieces:(n + 1) * pieces] for n in range(6)]
    g = refs[6 * pieces:6 * pieces + 4]
    out, lhs, rhs, sem, rsem = refs[-5:]
    i, n = pl.program_id(0), pl.num_programs(0)
    bm = out.shape[0]
    depth = g[0].shape[0]
    per = imp_h[0].shape[1] // bm
    diag = lax.axis_index("row") == lax.axis_index("col")

    def put(src, col, slot, k):
        return pltpu.make_async_copy(src.at[:, pl.ds(pl.multiple_of(col * bm, bm), bm)], lhs.at[slot, pl.ds(k * depth, depth)], sem.at[slot, k])

    def fetch(t):
        slot = lax.rem(t, 2)
        for j in range(pieces):
            @pl.when(t // per == j)
            def _():
                put(oth_h[j], lax.rem(t, per), slot, 1).start()
                put(oth_t[j], lax.rem(t, per), slot, 3).start()

            @pl.when(jnp.logical_and(t // per == j, diag))
            def _():
                put(act_h[j], lax.rem(t, per), slot, 0).start()
                put(act_t[j], lax.rem(t, per), slot, 2).start()

            @pl.when(jnp.logical_and(t // per == j, jnp.logical_not(diag)))
            def _():
                put(imp_h[j], lax.rem(t, per), slot, 0).start()
                put(imp_t[j], lax.rem(t, per), slot, 2).start()

    @pl.when(i == 0)
    def _():
        fetch(i)
        loads = [pltpu.make_async_copy(x, rhs.at[pl.ds(k * depth, depth)], rsem.at[k]) for k, x in enumerate(g)]
        for c in loads:
            c.start()
        for c in loads:
            c.wait()

    @pl.when(i + 1 < n)
    def _():
        fetch(i + 1)

    slot = lax.rem(i, 2)
    for k in range(4):
        put(act_h[0], 0, slot, k).wait()
    out[...] = lax.dot_general(lhs[slot], rhs[...], TN, preferred_element_type=jnp.float32)


def down_grad(act_h, act_t, imp_h, imp_t, oth_h, oth_t, gs, part, before, bm=512):
    pieces = len(imp_h)
    depth, n = gs[0].shape
    m = pieces * act_h[0].shape[1]
    ops = [*act_h, *act_t, *imp_h, *imp_t, *oth_h, *oth_t, *gs]
    aliases = {}
    if before is not None:
        aliases = {len(ops): 0}
        ops.append(before)
    steps = m // bm
    return pl.pallas_call(
        functools.partial(down_kernel, pieces),
        grid=(steps,),
        out_shape=jax.ShapeDtypeStruct((m * PARTS, n), F32),
        in_specs=[ANY] * len(ops),
        out_specs=pl.BlockSpec((bm, n), lambda i: (i + part * steps, 0)),
        scratch_shapes=[
            pltpu.VMEM((2, 4 * depth, bm), BF16),
            pltpu.VMEM((4 * depth, n), BF16),
            pltpu.SemaphoreType.DMA((2, 4)),
            pltpu.SemaphoreType.DMA((4,)),
        ],
        input_output_aliases=aliases,
        compiler_params=params(),
        cost_estimate=cost(m, n, 4 * depth),
        name="down_grad",
    )(*ops)


def params():
    return pltpu.CompilerParams(vmem_limit_bytes=60 << 20, dimension_semantics=("arbitrary",))


def load(copies):
    @pl.when(pl.program_id(0) == 0)
    def _():
        for c in copies:
            c.start()
        for c in copies:
            c.wait()


def place(src, dst, sem):
    return pltpu.make_async_copy(src, dst, sem)


def forward_kernel(x, x1, w, *refs):
    acts, (slope, lhs, sem) = refs[:PIECES], refs[PIECES:]
    half = x.shape[1]
    col = lax.axis_index("col")
    at = lambda k: lhs.at[:, pl.ds(pl.multiple_of(k * half, half), half)]
    load([place(x, at(col), sem.at[0]), place(x1, at(1 - col), sem.at[1])])
    u = lax.dot_general(lhs[...], w[...], NN, preferred_element_type=F32)
    cdf = 0.5 * (1.0 + lax.erf(u * INV_ROOT_TWO))
    slope[...] = cdf + u * jnp.exp(-0.5 * u * u) * INV_ROOT_TAU
    act = (u * cdf).astype(BF16)
    per = pl.num_programs(0) // PIECES
    for j, a in enumerate(acts):
        @pl.when(pl.program_id(0) // per == j)
        def _(a=a):
            a[...] = act


def forward(x, x1, w, bn=512):
    t, _ = x.shape
    h, f = w.shape
    per = f // bn // PIECES
    *acts, slope = pl.pallas_call(
        forward_kernel,
        grid=(f // bn,),
        out_shape=[jax.ShapeDtypeStruct((t, f // PIECES), BF16)] * PIECES + [jax.ShapeDtypeStruct((t, f), F32)],
        in_specs=[ANY, ANY, pl.BlockSpec((h, bn), lambda i: (0, i))],
        out_specs=[pl.BlockSpec((t, bn), lambda i, j=j: (0, jnp.clip(i - j * per, 0, per - 1))) for j in range(PIECES)]
        + [pl.BlockSpec((t, bn), lambda i: (0, i))],
        scratch_shapes=[pltpu.VMEM((t, h), BF16), pltpu.SemaphoreType.DMA((2,))],
        compiler_params=params(),
        cost_estimate=cost(t, f, h),
        name="forward",
    )(x, x1, w)
    return acts, slope


def backward_kernel(s, g, g1, wc, wa, wb, slope, out, lhs, sem):
    half = g.shape[1]
    sub = half // 2
    layer = lax.axis_index("depth")
    cut = lambda k: g1.at[:, pl.ds(pl.multiple_of(k * sub, sub), sub)]
    load([
        place(g, lhs.at[:, pl.ds(0, half)], sem.at[0]),
        place(cut(layer), lhs.at[:, pl.ds(half, sub)], sem.at[1]),
        place(cut(1 - layer), lhs.at[:, pl.ds(half + sub, sub)], sem.at[2]),
    ])
    d = lax.dot_general(lhs[:, :half], wc[...], NT, preferred_element_type=F32)
    d = d + lax.dot_general(lhs[:, half:half + sub], wa[...], NT, preferred_element_type=F32)
    d = d + lax.dot_general(lhs[:, half + sub:], wb[...], NT, preferred_element_type=F32)
    out[...] = (d * slope[...]).astype(BF16)


def backward(s, g, g1, down_g, down_a, down_b, slope, bn=512):
    t, half = g.shape
    f = slope.shape[1]
    steps = f // bn
    return pl.pallas_call(
        backward_kernel,
        grid_spec=pltpu.PrefetchScalarGridSpec(
            num_scalar_prefetch=1,
            grid=(steps,),
            in_specs=[
                ANY, ANY,
                pl.BlockSpec((bn, half), lambda i, s: (s[0] * steps + i, 0)),
                pl.BlockSpec((bn, half // 2), lambda i, s: (i, 0)),
                pl.BlockSpec((bn, half // 2), lambda i, s: (i, 0)),
                pl.BlockSpec((t, bn), lambda i, s: (0, i)),
            ],
            out_specs=pl.BlockSpec((t, bn), lambda i, s: (0, i)),
            scratch_shapes=[pltpu.VMEM((t, 2 * half), BF16), pltpu.SemaphoreType.DMA((3,))],
        ),
        out_shape=jax.ShapeDtypeStruct((t, f), BF16),
        compiler_params=params(),
        cost_estimate=cost(t, f, 2 * half),
        name="backward",
    )(s, g, g1, down_g, down_a, down_b, slope)


def row_kernel(dims, count, s, *refs):
    srcs, w, rest = refs[:count], refs[count], refs[count + 1:]
    add = rest[0] if len(rest) == 4 else None
    out, lhs, sem = rest[-3:]
    width = srcs[0].shape[1]
    load([place(x, lhs.at[:, pl.ds(k * width, width)], sem.at[k]) for k, x in enumerate(srcs)])
    r = lax.dot_general(lhs[...], w[...], dims, preferred_element_type=F32)
    if add is not None:
        r = r + add[...]
    out[...] = r.astype(out.dtype)


def row_product(s, srcs, w, add, half, dims, bn=256):
    t = srcs[0].shape[0]
    f = srcs[0].shape[1] * len(srcs)
    steps = half // bn
    if dims is NT:
        wspec = pl.BlockSpec((bn, f), lambda i, s: (s[0] * steps + i, 0))
    else:
        wspec = pl.BlockSpec((f, bn), lambda i, s: (s[0], i))
    tile = pl.BlockSpec((t, bn), lambda i, s: (0, i))
    return pl.pallas_call(
        functools.partial(row_kernel, dims, len(srcs)),
        grid_spec=pltpu.PrefetchScalarGridSpec(
            num_scalar_prefetch=1,
            grid=(steps,),
            in_specs=[ANY] * len(srcs) + [wspec] + ([] if add is None else [tile]),
            out_specs=tile,
            scratch_shapes=[pltpu.VMEM((t, f), BF16), pltpu.SemaphoreType.DMA((len(srcs),))],
        ),
        out_shape=jax.ShapeDtypeStruct((t, half), F32 if add is None else BF16),
        compiler_params=params(),
        cost_estimate=cost(t, half, f),
        name="row_product",
    )(s, *srcs, w, *([] if add is None else [add]))


def swap(x, axis):
    return lax.ppermute(x, axis, SWAP)


def solution(mesh):
    act_spec = P(("depth", "row"), "col")
    wgt_spec = P("row", "col")

    def grid_block(tok, up, down, grad):
        layer, col, row = lax.axis_index("depth"), lax.axis_index("col"), lax.axis_index("row")
        half = tok.shape[1]
        wide = up.shape[1]
        diag = row == col
        here = jnp.full((1,), col, jnp.int32)
        away = 1 - here

        q = wide // 2
        sub = lax.dynamic_slice(down, (row * q, layer * (half // 2)), (q, half // 2))
        oth = swap(lax.dynamic_slice(down, ((1 - row) * q, layer * (half // 2)), (q, half // 2)), "row")
        piece = jnp.where(diag, oth, sub)

        tok_1 = swap(tok, "col")
        tok_2 = swap(tok, "depth")
        grad_1 = swap(grad, "col")
        grad_2 = swap(grad, "depth")
        up_g = lax.all_gather(up, "row", axis=0, tiled=True)
        down_g = lax.all_gather(down, "row", axis=0, tiled=True)
        e = q // 2
        p1a, p1b = swap(piece[:e], "col"), swap(piece[e:], "col")
        p2a, p2b = swap(p1a, "depth"), swap(p1b, "depth")
        p1, p2 = jnp.concatenate([p1a, p1b], 0), jnp.concatenate([p2a, p2b], 0)
        tok_3 = swap(tok_1, "depth")
        grad_3 = swap(grad_1, "depth")
        down_a = lax.all_gather(p1, "row", axis=0, tiled=True)
        down_b = lax.all_gather(p2, "row", axis=0, tiled=True)

        act_h, slope_h = forward(tok, tok_1, up_g)
        act_t, slope_t = forward(tok_2, tok_3, up_g)
        imp_h = [swap(act_h[j], "col") for j in range(PIECES)]
        imp_t = [swap(imp_h[j], "depth") for j in range(PIECES)]

        du_h = backward(here, grad, grad_1, down_g, down_a, down_b, slope_h)
        sent = swap(row_product(away, [du_h], up_g, None, half, NT), "col")
        grad_tok = row_product(here, [du_h], up_g, sent, half, NT)
        du_t = backward(here, grad_2, grad_3, down_g, down_a, down_b, slope_t)

        pick = lambda a, b, k: jnp.where(k == col, a, b)
        flip = lambda x: jnp.swapaxes(x, 0, 1)
        tok_mh, tok_mt = flip(pick(tok, tok_1, row)), flip(pick(tok_2, tok_3, row))
        tok_sh = swap(flip(pick(tok, tok_1, 1 - row)), "row")
        tok_st = swap(flip(pick(tok_2, tok_3, 1 - row)), "row")
        du_sh, du_st = swap(du_h, "row"), swap(du_t, "row")
        up_sum = up_grad([tok_mh, tok_mt, tok_sh, tok_st], [du_h, du_t, du_sh, du_st])

        out = row_product(here, act_h, down_g, None, half, NN)
        out = row_product(away, imp_h, down_g, out, half, NN)

        grads = [grad, swap(grad, "row"), grad_2, swap(grad_2, "row")]
        oth_h = [swap(jnp.where(diag, imp_h[j], act_h[j]), "row") for j in range(PIECES)]
        oth_t = [swap(jnp.where(diag, imp_t[j], act_t[j]), "row") for j in range(PIECES)]
        down_sum = None
        per = PIECES // PARTS
        for n in range(PARTS):
            cut = lambda xs: xs[n * per:(n + 1) * per]
            down_sum = down_grad(cut(act_h), cut(act_t), cut(imp_h), cut(imp_t), cut(oth_h), cut(oth_t), grads, n, down_sum)
        return out, grad_tok, up_sum, down_sum

    return jax.shard_map(grid_block, mesh=mesh, in_specs=(act_spec, wgt_spec, wgt_spec, act_spec), out_specs=(act_spec, act_spec, wgt_spec, wgt_spec), check_vma=False)
```
